32 devices in a mesh: dp: 16 (over z, y, x), rep: 2 (over core).
Axes of the slice: x: 2, y: 2, z: 4, core: 2. Of those that a mesh axis runs over, the one named last changes fastest.
Arguments:
- tokens: bfloat16 [2, 1024, 4096], P('rep'), may hold values from -6 to 6
- cotangent: bfloat16 [2, 1024, 4096], P('rep'), may hold values from -6 to 6
- lengths: int32 [2, 2], P('rep'), may hold values from 1 to 512
- w_in: bfloat16 [4096, 2, 14336], P(None, None, 'dp'), may hold values from -0.09375 to 0.09375
- w_down: bfloat16 [14336, 4096], P('dp'), may hold values from -0.046875 to 0.046875
Outputs:
- d_tokens: float32 [2, 1024, 4096], P('rep', 'dp')
- weight_grads: float32 [4096, 3, 14336], P('rep', None, 'dp')
The draws below stay inside these ranges and needn't reach their ends.
All inputs are finite; a program needn't handle non-finite values.
Results may differ from the reference program's by a relative error of at most 0.0029.
Values sent between devices are 32-bit elements; how exact they have to be, the bound alone decides.
A program may use at most 256 MiB of HBM per device.

```python
import jax
import jax.numpy as jnp

D = 4096
HID = 14336
ROWS = 1024
SEQS = 2
SLOTS = 512
N_REP = 2


def with_ends(entries, rng, low, high):
    place = [jax.random.randint(jax.random.fold_in(rng, axis), (), 0, length) for axis, length in enumerate(entries.shape)]
    longest = entries.shape.index(max(entries.shape))
    beside = place[:longest] + [(place[longest] + 1) % entries.shape[longest]] + place[longest + 1:]
    return entries.at[tuple(place)].set(low).at[tuple(beside)].set(high)


def levels(rng, extent, cuts, low, largest):
    def one(dim, shards_of):
        draws = jax.random.uniform(jax.random.fold_in(jax.random.fold_in(rng, 6), dim), (shards_of,), jnp.float32, low / len(cuts), largest / len(cuts))
        return jnp.repeat(jnp.exp(draws), extent[dim] // shards_of).reshape((-1,) + (1,) * (len(extent) - dim - 1))

    loudness = one(*cuts[0])
    for cut in cuts[1:]:
        loudness = loudness * one(*cut)
    return loudness


def centred(stream_key, dims, scale, bound, cuts=(), kind=jnp.bfloat16):
    values = scale * jax.random.normal(stream_key, dims, jnp.float32)
    if cuts:
        values = values * levels(stream_key, dims, cuts, -0.22, 0.18)
    return jnp.clip(values, -bound, bound).astype(kind)


def setup_inputs(seed: int = 0) -> dict:
    key_list = jax.random.split(jax.random.key(seed), 6)
    return {
        "tokens": centred(key_list[0], (N_REP, ROWS, D), 1.0, 6.0, ((0, 2),)),
        "cotangent": centred(key_list[1], (N_REP, ROWS, D), 1.0, 6.0, ((0, 2),)),
        "lengths": with_ends(jax.random.randint(key_list[2], (N_REP, SEQS), 1, SLOTS + 1), jax.random.fold_in(key_list[2], 1), 1, SLOTS).astype(jnp.int32),
        "w_in": centred(key_list[3], (D, 2, HID), D ** -0.5, 0.09375, ((2, 16),)),
        "w_down": centred(key_list[4], (HID, D), HID ** -0.5, 0.046875, ((0, 16),)),
    }


GRAD_SCALE = 0.03125


def reference(tokens, cotangent, lengths, w_in, w_down):
    hidden_units = w_down.shape[0]
    slots = ROWS // SEQS
    position = jnp.arange(ROWS)
    w_flat = w_in.reshape(D, 2 * hidden_units)
    zero_value = jnp.zeros((), jnp.bfloat16)
    total = jnp.zeros((D, 3, hidden_units), jnp.float32)
    results = []
    for replica in range(N_REP):
        limit = lengths[replica][position // slots]
        is_alive = (position % slots) < limit
        live_x = jnp.where(is_alive[:, None], tokens[replica], zero_value)
        live_dy = jnp.where(is_alive[:, None], cotangent[replica], zero_value)
        gate_up = jnp.dot(live_x, w_flat, preferred_element_type=jnp.float32)
        gate = gate_up[:, :hidden_units]
        upward = gate_up[:, hidden_units:]
        sigmoid_gate = jax.nn.sigmoid(gate)
        activated = gate * sigmoid_gate
        hidden = (activated * upward).astype(jnp.bfloat16)
        d_hidden = jnp.dot(live_dy, w_down.T, preferred_element_type=jnp.float32)
        d_gate = d_hidden * upward * sigmoid_gate * (1.0 + gate * (1.0 - sigmoid_gate))
        d_up = d_hidden * activated
        d_in = jnp.concatenate([d_gate, d_up], axis=1).astype(jnp.bfloat16)
        results.append(jnp.dot(d_in, w_flat.T, preferred_element_type=jnp.float32))
        grad_in = jnp.dot(live_x.T, d_in, preferred_element_type=jnp.float32)
        grad_down = jnp.dot(live_dy.T, hidden, preferred_element_type=jnp.float32)
        combined = jnp.concatenate([grad_in.reshape(D, 2, hidden_units), grad_down[:, None, :]], axis=1)
        total = total + combined * GRAD_SCALE
    return jnp.stack(results), total
```

```python
import jax
import jax.numpy as jnp
from jax import lax
from jax.experimental import pallas as pl
from jax.experimental.pallas import tpu as pltpu
from jax.sharding import PartitionSpec as P

GRAD_SCALE = 0.03125
COPIES_PER_ORDER = 2


def cube_code(index, bits):
    if bits < 2:
        return index
    return index ^ ((index >> 1) & (1 << (bits - 2)))


def bit_slice(blocks, axis, value):
    return lax.index_in_dim(blocks, value, axis, keepdims=False)


def copy_block(owners_ref, src_ref, dst_ref):
    dst_ref[...] = src_ref[...]


def reorder(owners, d_in, share):
    n_dp = owners.shape[0]
    width = d_in.shape[1]
    return pl.pallas_call(
        copy_block,
        out_shape=jax.ShapeDtypeStruct(d_in.shape, d_in.dtype),
        grid_spec=pltpu.PrefetchScalarGridSpec(
            num_scalar_prefetch=1,
            grid=(n_dp,),
            in_specs=[pl.BlockSpec((share, width), lambda i, owners: (owners[i], 0))],
            out_specs=pl.BlockSpec((share, width), lambda i, owners: (i, 0)),
        ),
        cost_estimate=pl.CostEstimate(
            flops=0, bytes_accessed=4 * d_in.size, transcendentals=0
        ),
        compiler_params=pltpu.CompilerParams(vmem_limit_bytes=8 * 2**20),
    )(owners, d_in)


def per_device(n_dp, n_rep, tokens, cotangent, lengths, w_in, w_down):
    rows = tokens.shape[1]
    width = tokens.shape[2]
    seqs = lengths.shape[1]
    slots = rows // seqs
    hidden_units = w_down.shape[0]
    bits = n_dp.bit_length() - 1
    share = rows // n_dp
    position = jnp.arange(rows)
    owner_seq = (position // slots)[:, None] == jnp.arange(seqs)[None, :]
    limit = jnp.sum(jnp.where(owner_seq, lengths[0][None, :], 0), axis=1)
    is_alive = position % slots < limit
    zero_value = jnp.zeros((), jnp.bfloat16)
    live_x = jnp.where(is_alive[:, None], tokens[0], zero_value)
    live_dy = jnp.where(is_alive[:, None], cotangent[0], zero_value)
    w_flat = lax.optimization_barrier(w_in.reshape(width, 2 * hidden_units))
    gate_up = jnp.dot(live_x, w_flat, preferred_element_type=jnp.float32)
    gate = gate_up[:, :hidden_units]
    upward = gate_up[:, hidden_units:]
    sigmoid_gate = jax.nn.sigmoid(gate)
    activated = gate * sigmoid_gate
    hidden = (activated * upward).astype(jnp.bfloat16)
    d_hidden = lax.dot_general(
        live_dy, w_down, (((1,), (1,)), ((), ())), preferred_element_type=jnp.float32
    )
    d_gate = d_hidden * upward * sigmoid_gate * (1.0 + gate * (1.0 - sigmoid_gate))
    d_up = d_hidden * activated
    d_in = jnp.concatenate([d_gate, d_up], axis=1).astype(jnp.bfloat16)

    me = lax.axis_index("dp")
    my_code = cube_code(me, bits)
    owners = cube_code(my_code ^ jnp.arange(n_dp, dtype=jnp.int32), bits)
    blocks = reorder(owners, d_in, share)
    blocks = blocks.reshape((2,) * bits + (share, 2 * hidden_units))

    n_chunks = bits * COPIES_PER_ORDER
    while width % n_chunks:
        n_chunks -= 1
    columns = width // n_chunks
    flows = []
    for chunk in range(n_chunks):
        order = [(chunk + step) % bits for step in range(bits)]
        weights = lax.slice_in_dim(w_flat, chunk * columns, (chunk + 1) * columns, axis=0)

        def product(part, weights=weights):
            return lax.dot_general(
                part, weights, (((part.ndim - 1,), (1,)), ((), ())), preferred_element_type=jnp.float32
            )

        axis = bits - 1 - order[0]
        sent = product(bit_slice(blocks, axis, 1))
        kept = product(bit_slice(blocks, axis, 0))
        flows.append((order, sent, kept))

    def partner_pairs(bit):
        return [(d, cube_code(cube_code(d, bits) ^ (1 << bit), bits)) for d in range(n_dp)]

    part = width // n_rep
    rep = lax.axis_index("rep")

    def gradients(owner, after):
        x_all, dy_all, d_all, h_all, _ = lax.optimization_barrier((live_x, live_dy, d_in, hidden, after))
        x_part = lax.dynamic_slice_in_dim(x_all, owner * part, part, 1)
        dy_part = lax.dynamic_slice_in_dim(dy_all, owner * part, part, 1)
        pairs = (
            (x_part, d_all[:, :hidden_units]),
            (x_part, d_all[:, hidden_units:]),
            (dy_part, h_all),
        )
        return lax.optimization_barrier(
            tuple(
                lax.dot_general(
                    rows_of, units, (((0,), (0,)), ((), ())), preferred_element_type=jnp.float32
                )
                for rows_of, units in pairs
            )
        )

    first_sent = tuple(sent for _, sent, _ in flows)
    totals = [[], [], []]
    for shift in range(1, n_rep):
        ring = [(r, (r + shift) % n_rep) for r in range(n_rep)]
        for kind, grad in enumerate(gradients((rep + shift) % n_rep, first_sent)):
            totals[kind].append(lax.ppermute(grad, "rep", ring))

    results = [None] * n_chunks
    state = {}
    for chunk, (order, sent, kept) in enumerate(flows):
        state[chunk] = (sent, kept, sorted(order, reverse=True))
    shared = None
    for step in range(bits):
        if step == 1:
            own = gradients(rep, tuple(state[chunk][0] for chunk in range(min(bits, n_chunks))))
            for kind in range(3):
                totals[kind].append(own[kind])
            shared = jnp.stack([sum(terms[1:], terms[0]) for terms in totals], axis=1) * GRAD_SCALE
        for chunk in range(n_chunks):
            order = flows[chunk][0]
            sent, kept, left = state[chunk]
            if step == bits - 1 and shared is not None and chunk >= n_chunks // 2:
                sent, _ = lax.optimization_barrier((sent, shared))
            got = lax.ppermute(sent, "dp", partner_pairs(order[step]))
            left = [b for b in left if b != order[step]]
            if step == bits - 1:
                results[chunk] = kept + got
            else:
                axis = left.index(order[step + 1])
                sent = bit_slice(kept, axis, 1) + bit_slice(got, axis, 1)
                kept = bit_slice(kept, axis, 0) + bit_slice(got, axis, 0)
                state[chunk] = (sent, kept, left)
    shard = jnp.concatenate(results, axis=1)
    return (shard[None], shared)


def solution(mesh):
    n_dp = mesh.shape["dp"]
    n_rep = mesh.shape["rep"]

    def body(*args):
        return per_device(n_dp, n_rep, *args)

    in_specs = (
        P("rep", None, None),
        P("rep", None, None),
        P("rep", None),
        P(None, None, "dp"),
        P("dp", None),
    )
    out_specs = (P("rep", "dp", None), P("rep", None, "dp"))
    return jax.shard_map(
        body, mesh=mesh, in_specs=in_specs, out_specs=out_specs, check_vma=False
    )
```
